128 devices in a mesh: dom: 32 (over y, x, core), dim: 4 (over z).
Axes of the slice: x: 4, y: 4, z: 4, core: 2. Of those that a mesh axis runs over, the one named last changes fastest.
Arguments:
- particles: float32 [256, 1024], P('dom', 'dim'), may hold values from -5 to 5
- data_rows: bfloat16 [256, 16, 1024], P('dom', None, 'dim'), may hold values from -0.375 to 0.375
- labels: int32 [256, 16], P('dom'), may hold values from 0 to 1
Outputs:
- updates: float32 [2, 256, 1024], P(None, 'dom', 'dim')
The draws below stay inside these ranges and needn't reach their ends.
All inputs are finite; a program needn't handle non-finite values.
Results may differ from the reference program's by a relative error of at most 0.0003.
Values may be sent and summed in bfloat16 or wider, within the bound.
A program may use at most 64 MiB of HBM per device.

```python
import math
import jax
import jax.numpy as jnp
from jax import lax

D = 1024
R = 16
NEWTON = 2
CG_STEPS = 2
BAND = 1
PARTICLES = 256


def draw_particles(key, part):
    scale_key, value_key = jax.random.split(key, 2)
    spread = jnp.exp(jax.random.uniform(scale_key, (PARTICLES, 1), jnp.float32, math.log(0.4), math.log(1.1)))
    values = jax.random.truncated_normal(value_key, -4.0, 4.0, (PARTICLES, D), jnp.float32)
    return spread * values


def touch_ends(result, key, least, largest):
    shape = result.shape
    spot = [jax.random.randint(jax.random.fold_in(key, axis), (), 0, shape[axis]) for axis in range(len(shape))]
    result = result.at[tuple(spot)].set(least)
    longest = shape.index(max(shape))
    spot[longest] = (spot[longest] + 1) % shape[longest]
    return result.at[tuple(spot)].set(largest)


def shard_levels(rng, dims, shards, least, top_value):
    def one(axis_at, parts):
        heights = jax.random.uniform(jax.random.fold_in(jax.random.fold_in(rng, 6), axis_at), (parts,), jnp.float32, least / len(shards), top_value / len(shards))
        return jnp.repeat(jnp.exp(heights), dims[axis_at] // parts).reshape((-1,) + (1,) * (len(dims) - axis_at - 1))

    loudness = one(*shards[0])
    for cut in shards[1:]:
        loudness = loudness * one(*cut)
    return loudness


def noise(key, dims, width, limit, shards=(), kind=jnp.bfloat16):
    array = jax.random.normal(key, dims, jnp.float32) * width
    if len(shards) > 0:
        array = shard_levels(key, dims, shards, -0.22, 0.18) * array
    return jnp.clip(array, min=-limit, max=limit).astype(kind)


def setup_inputs(seed: int = 0) -> dict:
    keys = jax.random.split(jax.random.key(seed), 4)
    particles = draw_particles(jax.random.fold_in(keys[3], 71), 0)
    data_rows = noise(keys[1], (PARTICLES, R, D), (D // 4) ** -0.5, 0.375, ((0, 32), (2, 4)))
    labels = touch_ends(jax.random.randint(keys[2], (PARTICLES, R), 0, 2), jax.random.fold_in(keys[2], 1), 0, 1).astype(jnp.int32)
    return {"particles": particles, "data_rows": data_rows, "labels": labels}


prior_precision = 0.05
like_weight = 4.0
move_size = 0.5
highest = lax.Precision.HIGHEST


def reference(particles, data_rows, labels):
    factor_rows = data_rows.astype(jnp.float32)
    targets = labels.astype(jnp.float32)
    count = particles.shape[0]
    kernel_scale = 1.0 * BAND * D
    cross_scale = 4.0 / (kernel_scale * kernel_scale)
    current = particles
    outputs = []
    for newton_step in range(NEWTON):
        logits = jnp.einsum("jrd,jd->jr", factor_rows, current, precision=highest)
        probs = jax.nn.sigmoid(logits)
        gradient = -prior_precision * current + like_weight * jnp.einsum("jr,jrd->jd", targets - probs, factor_rows, precision=highest)
        curvature = like_weight * probs * (1.0 - probs)
        squares = jnp.sum(current * current, axis=1)
        inner_rows = jnp.dot(current, current.T, precision=highest)
        distance = squares[:, None] + squares[None, :] - 2.0 * inner_rows
        kernel = jnp.exp(-distance / kernel_scale)
        kernel_sq = kernel * kernel
        kernel_total = jnp.sum(kernel, axis=1)
        square_total = jnp.sum(kernel_sq, axis=1)
        kernel_grad = jnp.dot(kernel, gradient, precision=highest)
        kernel_pos = jnp.dot(kernel, current, precision=highest)
        square_pos = jnp.dot(kernel_sq, current, precision=highest)
        drift = (kernel_grad + (2.0 / kernel_scale) * (current * kernel_total[:, None] - kernel_pos)) / count

        def apply_operator(vectors):
            along_self = jnp.sum(current * vectors, axis=1)
            along_mean = jnp.sum(vectors * square_pos, axis=1)
            projected = jnp.einsum("jrd,id->jri", factor_rows, vectors, precision=highest)
            weighted = projected * curvature[:, :, None] * kernel_sq.T[:, None, :]
            pairs = jnp.einsum("jrd,jri->id", factor_rows, weighted, precision=highest)
            along_pair = jnp.dot(current, vectors.T, precision=highest)
            pairs = pairs + cross_scale * jnp.dot((kernel_sq.T * along_pair).T, current, precision=highest)
            local = prior_precision * square_total[:, None] * vectors + cross_scale * (current * (along_self * square_total - along_mean)[:, None] - along_self[:, None] * square_pos)
            return (pairs + local) / count

        solution = jnp.zeros_like(drift)
        residual = drift
        direction = drift
        norm_now = jnp.sum(residual * residual)
        for solve_step in range(CG_STEPS):
            image = apply_operator(direction)
            alpha = norm_now / jnp.sum(direction * image)
            solution = solution + alpha * direction
            residual = residual - alpha * image
            if solve_step + 1 < CG_STEPS:
                norm_next = jnp.sum(residual * residual)
                direction = residual + (norm_next / norm_now) * direction
                norm_now = norm_next
        outputs.append(solution)
        current = current + move_size * solution
    return jnp.stack(outputs)
```

```python
import jax
import jax.numpy as jnp
from jax import lax
from jax.experimental import pallas as pl
from jax.experimental.pallas import tpu as pltpu
from jax.sharding import Mesh, PartitionSpec as P

DIMS = ("y", "x", "z")
THIRDS = ((("x", "y", "z"), 0, 3), (("y", "z", "x"), 3, 3), (("z", "x", "y"), 6, 2))
AX = ("dom_0", "dom_1", "dom_2", "dim")

def gather_kernel(a_in, xl_in, a_out, xl_out, A, XL, loc, send, recv, osem):
    y, x, c, z = (lax.axis_index(n) for n in AX)
    me = {"y": y, "x": x, "z": z}

    def shift(dim, k):
        return lax.rem(me[dim] + 4 + k, 4)

    def dev(dim, k):
        p = dict(me)
        p[dim] = shift(dim, k)
        return (p["y"], p["x"], c, p["z"])

    def a_slice(third, sel, half=None):
        _, j0, nj = THIRDS[third]
        ys = pl.ds(sel["y"], 1) if "y" in sel else slice(None)
        xs = pl.ds(sel["x"], 1) if "x" in sel else slice(None)
        if "z" in sel:
            w = 256 if half is None else 128
            st = pl.multiple_of(sel["z"] * 256 + (0 if half is None else half * 128), 128)
        else:
            w = 1024 if half is None else 512
            st = 0 if half is None else half * 512
        return A.at[ys, xs, pl.ds(j0, nj), :, pl.ds(st, w)]

    def x_slice(third, sel, half=None):
        ys = pl.ds(sel["y"], 1) if "y" in sel else slice(None)
        xs = pl.ds(sel["x"], 1) if "x" in sel else slice(None)
        if "z" in sel:
            return XL.at[third, ys, xs, :, pl.ds(pl.multiple_of(sel["z"] * 128, 128), 128)]
        return XL.at[third, ys, xs]

    counter = [0]
    pending = []

    def new():
        counter[0] += 1
        return counter[0] - 1

    def copy(ref, target, s):
        return pltpu.make_async_remote_copy(src_ref=ref, dst_ref=ref, send_sem=send.at[s], recv_sem=recv.at[s], device_id=target, device_id_type=pl.DeviceIdType.MESH)

    class Group:
        def __init__(self, slicer, third, dim, rest, halves):
            self.f, self.t, self.dim, self.rest, self.halves = slicer, third, dim, rest, halves
            self.s = [new() for _ in range(4 if halves else 3)]

        def ref(self, k, half=None):
            sel = dict(self.rest)
            sel[self.dim] = shift(self.dim, k)
            return self.f(self.t, sel, half)

        def start(self):
            for k, s in ((1, 0), (-1, 1)):
                d = copy(self.ref(0), dev(self.dim, k), self.s[s]); d.start(); pending.append(d)

        def got(self, k):
            s = self.s[0 if k == -1 else 1]
            copy(self.ref(k), dev(self.dim, k), s).wait_recv()
            if k == -1:
                h = 0 if self.halves else None
                d = copy(self.ref(-1, h), dev(self.dim, 1), self.s[2]); d.start(); pending.append(d)
            elif self.halves:
                d = copy(self.ref(1, 1), dev(self.dim, -1), self.s[3]); d.start(); pending.append(d)

        def far(self):
            copy(self.ref(2, 0 if self.halves else None), dev(self.dim, -1), self.s[2]).wait_recv()
            if self.halves:
                copy(self.ref(2, 1), dev(self.dim, 1), self.s[3]).wait_recv()

    own = (pl.ds(y, 1), pl.ds(x, 1))
    l1 = pltpu.make_async_copy(a_in, A.at[y, x, :, :, pl.ds(pl.multiple_of(z * 256, 256), 256)], loc.at[0])
    l1.start()
    l2s = []
    for t in range(3):
        l2 = pltpu.make_async_copy(xl_in.at[t], XL.at[t, y, x, :, pl.ds(pl.multiple_of(z * 128, 128), 128)], loc.at[1 + t])
        l2.start(); l2s.append(l2)
    barrier = pltpu.get_barrier_semaphore()
    for dim in DIMS:
        for k in (1, -1):
            pl.semaphore_signal(barrier, inc=1, device_id=dev(dim, k), device_id_type=pl.DeviceIdType.MESH)
    pl.semaphore_wait(barrier, 6)
    l1.wait()
    for l2 in l2s:
        l2.wait()

    T = range(3)
    order = [t[0] for t in THIRDS]
    XA = [Group(x_slice, t, order[t][0], {}, False) for t in T]
    for t in T:
        a, b, cc = order[t]
        XA[t].rest = {b: me[b], cc: me[cc]}
    XB = [Group(x_slice, t, order[t][1], {order[t][2]: me[order[t][2]]}, False) for t in T]
    XC = [Group(x_slice, t, order[t][2], {}, False) for t in T]
    for g in XA: g.start()
    GA = [Group(a_slice, t, order[t][0], {order[t][1]: me[order[t][1]], order[t][2]: me[order[t][2]]}, True) for t in T]
    OFF = (0, -1, 1, 2)
    GB = [[Group(a_slice, t, order[t][1], {order[t][0]: shift(order[t][0], o), order[t][2]: me[order[t][2]]}, True) for o in OFF] for t in T]
    GC = [[Group(a_slice, t, order[t][2], {order[t][0]: shift(order[t][0], o), order[t][1]: me[order[t][1]]}, True) for o in OFF] for t in T]
    GL = [[Group(a_slice, t, order[t][2], {order[t][1]: shift(order[t][1], o)}, True) for o in OFF[1:]] for t in T]
    for t in T: GA[t].start()
    for t in T: GB[t][0].start()
    for t in T: GC[t][0].start()
    for k, i in ((-1, 1), (1, 2)):
        for t in T: XA[t].got(k)
        for t in T: GA[t].got(k)
        for t in T: GB[t][i].start()
        for t in T: GC[t][i].start()
    for t in T:
        XA[t].far()
        XB[t].start()
    for k in (-1, 1):
        for t in T: GB[t][0].got(k)
    for t in T:
        GA[t].far()
        GB[t][3].start()
    for t in T: GC[t][3].start()
    for k in (-1, 1):
        for t in T: XB[t].got(k)
    for i in (1, 2):
        for k in (-1, 1):
            for t in T: GB[t][i].got(k)
    for t in T:
        XB[t].far()
        XC[t].start()
    for n, k in enumerate((-1, 1)):
        for t in T:
            GB[t][3].got(k)
            GL[t][n].start()
    for i in range(3):
        for k in (-1, 1):
            for t in T: GC[t][i].got(k)
    for t in T:
        for i in range(4): GB[t][i].far()
        GL[t][2].start()
    for k in (-1, 1):
        for t in T: XC[t].got(k)
    for k in (-1, 1):
        for t in T: GC[t][3].got(k)
    for i in range(3):
        for k in (-1, 1):
            for t in T: GL[t][i].got(k)
    for t in T: XC[t].far()
    for t in T:
        for g in GC[t] + GL[t]: g.far()
    for d in pending: d.wait_send()
    o1 = pltpu.make_async_copy(A, a_out, osem.at[0]); o1.start()
    o2 = pltpu.make_async_copy(XL, xl_out, osem.at[1]); o2.start()
    o1.wait(); o2.wait()

NSEM = 144 + 27

def gather(a, xl):
    return pl.pallas_call(
        gather_kernel,
        out_shape=(jax.ShapeDtypeStruct((4, 4, 8, 16, 1024), jnp.bfloat16), jax.ShapeDtypeStruct((3, 4, 4, 8, 512), jnp.float32)),
        in_specs=[pl.BlockSpec(memory_space=pl.ANY)] * 2,
        out_specs=(pl.BlockSpec(memory_space=pl.ANY),) * 2,
        scratch_shapes=[
            pltpu.VMEM((4, 4, 8, 16, 1024), jnp.bfloat16),
            pltpu.VMEM((3, 4, 4, 8, 512), jnp.float32),
            pltpu.SemaphoreType.DMA((4,)),
            pltpu.SemaphoreType.DMA((NSEM,)),
            pltpu.SemaphoreType.DMA((NSEM,)),
            pltpu.SemaphoreType.DMA((2,)),
        ],
        compiler_params=pltpu.CompilerParams(collective_id=0, has_side_effects=True, vmem_limit_bytes=60 << 20),
        name="gather",
    )(a, xl)


highest = lax.Precision.HIGHEST
DOM = AX[:3]


def ein(spec, *args):
    return jnp.einsum(spec, *args, precision=highest)


def per_device(particles, data_rows, labels):
    y, x, c, z = (lax.axis_index(n) for n in AX)
    xl = jnp.stack([particles[:, :128], particles[:, 128:], jnp.pad(labels.astype(jnp.float32), ((0, 0), (0, 112)))])
    A, XL = gather(data_rows, xl)
    A = A.reshape(128, 16, 1024)
    X = jnp.concatenate([XL[0].reshape(128, 4, 1, 128), XL[1].reshape(128, 4, 1, 128)], axis=2).reshape(128, 1024)
    T = XL[2].reshape(128, 512)[:, :16]
    Af = A.astype(jnp.float32)
    row = (y * 4 + x) * 8 + 2 * z
    mine = lax.axis_index("dom_2")

    def pair(v):
        return lax.psum(v, "dom_2")

    def shared(v2):
        return lax.psum(jnp.where((jnp.arange(2) == mine)[:, None, None], v2[None], 0.0), "dom_2").reshape(4, -1)

    outs = []
    for step in range(2):
        xi = shared(lax.dynamic_slice_in_dim(X, row, 2, 0))
        logits = ein("jrd,jd->jr", Af, X)
        p = jax.nn.sigmoid(logits)
        curv = 4.0 * p * (1.0 - p)
        d2 = jnp.sum(xi * xi, 1)[:, None] + jnp.sum(X * X, 1)[None] - 2.0 * ein("id,jd->ij", xi, X)
        K = jnp.exp(-d2 / 1024.0)
        K2 = K * K
        grad = -0.05 * X + 4.0 * ein("jr,jrd->jd", T - p, Af)
        b = pair(ein("ij,jd->id", K, grad) + (2.0 / 1024) * (xi * jnp.sum(K, 1)[:, None] - ein("ij,jd->id", K, X))) / 256.0

        def fwd(v):
            return ein("jrd,id->ijr", Af, v), jnp.sum(xi * v, 1)[:, None] - ein("jd,id->ij", X, v)

        def quad(v, P, Y):
            return (0.05 * jnp.sum(K2, 1)[:, None] * v * v).sum() + (K2[:, :, None] * curv[None] * P * P).sum() + (4.0 / 1024**2) * (K2 * Y * Y).sum()

        P1, Y1 = fwd(b)
        KY = K2 * Y1
        w = pair(0.05 * jnp.sum(K2, 1)[:, None] * b + ein("ijr,jrd->id", K2[:, :, None] * curv[None] * P1, Af)
                 + (4.0 / 1024**2) * (xi * jnp.sum(KY, 1)[:, None] - ein("ij,jd->id", KY, X))) / 256.0
        P2, Y2 = fwd(w)
        wu = quad(w, P2, Y2) / 256.0
        rr, bw, ww, wu = lax.psum(jnp.stack([jnp.sum(b * b) / 2, jnp.sum(b * w) / 2, jnp.sum(w * w) / 2, wu]), AX)
        a0 = rr / bw
        nn = rr - 2.0 * a0 * bw + a0 * a0 * ww
        beta = nn / rr
        den = (1 + beta) ** 2 * bw - 2 * (1 + beta) * a0 * ww + a0 * a0 * wu
        a1 = nn / den
        up = (a0 + a1 * (1 + beta)) * b - a1 * a0 * w
        mine2 = lax.dynamic_slice_in_dim(up, 2 * mine, 2, 0)
        sent = lax.all_to_all(mine2.reshape(2, 4, 256), "dim", split_axis=1, concat_axis=0, tiled=True)
        outs.append(sent.reshape(8, 256))
        if step == 0:
            full = mine2
            for name in ("dim", "dom_1", "dom_0"):
                full = lax.all_gather(full, name, axis=0, tiled=True)
            X = X + 0.5 * full
    return jnp.stack(outs)


def solution(mesh):
    torus = Mesh(mesh.devices.reshape(4, 4, 2, mesh.shape["dim"]), AX)
    return jax.shard_map(per_device, mesh=torus, in_specs=(P(DOM, "dim"), P(DOM, None, "dim"), P(DOM, None)), out_specs=P(None, DOM, "dim"), check_vma=False)
```

```python
import jax
import jax.numpy as jnp
from jax import lax
from jax.experimental import pallas as pl
from jax.experimental.pallas import tpu as pltpu
from jax.sharding import Mesh, PartitionSpec as P

DIMS = ("y", "x", "z")
THIRDS = ((("x", "y", "z"), 0, 3), (("y", "z", "x"), 3, 3), (("z", "x", "y"), 6, 2))
AX = ("dom_0", "dom_1", "dom_2", "dim")
DOM = AX[:3]
MESH = pl.DeviceIdType.MESH
F32, BF16 = jnp.float32, jnp.bfloat16
SCALE = 1024.0
CROSS = 4.0 / (SCALE * SCALE)
COUNT = 256.0
OFF = (0, -1, 1, 2)
NSEM = 260


def nn(a, b):
    return lax.dot_general(a, b, (((1,), (0,)), ((), ())), preferred_element_type=F32)


def nt(a, b):
    return lax.dot_general(a, b, (((1,), (1,)), ((), ())), preferred_element_type=F32)


def pieces(v, n):
    out = []
    for k in range(n):
        h = v.astype(BF16)
        out.append(h)
        if k + 1 < n:
            v = v - h.astype(F32)
    return out


def stacked(v, n):
    return jnp.concatenate(pieces(v, n), axis=0)


def folded(v, n):
    out = v[:8]
    for k in range(1, n):
        out = out + v[8 * k : 8 * k + 8]
    return out


def lane_parts(v):
    out = v[:, :128]
    for k in range(1, v.shape[1] // 128):
        out = out + v[:, 128 * k : 128 * k + 128]
    return out


def kernel(a_in, xl_in, out_ref, A, XL, X, XP, EX, BG, WG, BL, WL, PS, PR, SC, loc, send, recv):
    y, x, c, z = (lax.axis_index(n) for n in AX)
    me = {"y": y, "x": x, "z": z}
    partner = (y, x, 1 - c, z)

    def shift(dim, k):
        return lax.rem(me[dim] + 4 + k, 4)

    def dev(dim, k):
        p = dict(me)
        p[dim] = shift(dim, k)
        return (p["y"], p["x"], c, p["z"])

    def a_slice(third, sel, half=None):
        _, j0, nj = THIRDS[third]
        ys = pl.ds(sel["y"], 1) if "y" in sel else slice(None)
        xs = pl.ds(sel["x"], 1) if "x" in sel else slice(None)
        if "z" in sel:
            w = 256 if half is None else 128
            st = pl.multiple_of(sel["z"] * 256 + (0 if half is None else half * 128), 128)
        else:
            w = 1024 if half is None else 512
            st = 0 if half is None else half * 512
        return A.at[ys, xs, pl.ds(j0, nj), :, pl.ds(st, w)]

    def x_slice(third, sel, half=None):
        ys = pl.ds(sel["y"], 1) if "y" in sel else slice(None)
        xs = pl.ds(sel["x"], 1) if "x" in sel else slice(None)
        if "z" in sel:
            return XL.at[third, ys, xs, :, pl.ds(pl.multiple_of(sel["z"] * 128, 128), 128)]
        return XL.at[third, ys, xs]

    counter = [0]
    pending = []

    def new():
        counter[0] += 1
        return counter[0] - 1

    def copy(ref, target, s, dst=None):
        return pltpu.make_async_remote_copy(
            src_ref=ref, dst_ref=ref if dst is None else dst, send_sem=send.at[s], recv_sem=recv.at[s],
            device_id=target, device_id_type=MESH,
        )

    def go(d):
        d.start()
        pending.append(d)

    class Group:
        def __init__(self, slicer, third, dim, rest, halves):
            self.f, self.t, self.dim, self.rest, self.halves = slicer, third, dim, rest, halves
            self.s = [new() for _ in range(4 if halves else 3)]

        def ref(self, k, half=None):
            sel = dict(self.rest)
            sel[self.dim] = shift(self.dim, k)
            return self.f(self.t, sel, half)

        def start(self):
            for k, s in ((1, 0), (-1, 1)):
                go(copy(self.ref(0), dev(self.dim, k), self.s[s]))

        def got(self, k):
            s = self.s[0 if k == -1 else 1]
            copy(self.ref(k), dev(self.dim, k), s).wait_recv()
            if k == -1:
                go(copy(self.ref(-1, 0 if self.halves else None), dev(self.dim, 1), self.s[2]))
            elif self.halves:
                go(copy(self.ref(1, 1), dev(self.dim, -1), self.s[3]))

        def far(self):
            copy(self.ref(2, 0 if self.halves else None), dev(self.dim, -1), self.s[2]).wait_recv()
            if self.halves:
                copy(self.ref(2, 1), dev(self.dim, 1), self.s[3]).wait_recv()

    class Ring:
        def __init__(self, dim, at):
            self.dim, self.at = dim, at
            self.s = [new() for _ in range(3)]

        def start(self):
            for n, k in enumerate((1, 3, 2)):
                go(copy(self.at(me[self.dim]), dev(self.dim, k), self.s[n]))

        def wait(self):
            for n, k in enumerate((1, 3, 2)):
                copy(self.at(shift(self.dim, -k)), dev(self.dim, k), self.s[n]).wait_recv()

    n_pair = [0]

    class Pair:
        def __init__(self, value):
            self.value, self.n, self.s = value, n_pair[0], new()
            n_pair[0] += 1
            w = value.shape[1]
            PS[self.n, :, :w] = value
            self.d = copy(PS.at[self.n, :, pl.ds(0, w)], partner, self.s, PR.at[self.n, :, pl.ds(0, w)])
            go(self.d)
            self.w = w

        def total(self):
            self.d.wait_recv()
            return self.value + PR[self.n, :, : self.w]

    l1 = pltpu.make_async_copy(a_in, A.at[y, x, :, :, pl.ds(pl.multiple_of(z * 256, 256), 256)], loc.at[0])
    l1.start()
    l2s = []
    for t in range(3):
        l2 = pltpu.make_async_copy(xl_in.at[t], XL.at[t, y, x, :, pl.ds(pl.multiple_of(z * 128, 128), 128)], loc.at[1 + t])
        l2.start()
        l2s.append(l2)
    barrier = pltpu.get_barrier_semaphore()
    for dim in DIMS:
        for k in (1, 2, 3):
            pl.semaphore_signal(barrier, inc=1, device_id=dev(dim, k), device_id_type=MESH)
    pl.semaphore_signal(barrier, inc=1, device_id=partner, device_id_type=MESH)
    EX[...] = (lax.broadcasted_iota(jnp.int32, (128, 2048), 1) // 16 == lax.broadcasted_iota(jnp.int32, (128, 2048), 0)).astype(F32).astype(BF16)
    pl.semaphore_wait(barrier, 10)
    l1.wait()
    for l2 in l2s:
        l2.wait()

    T = range(3)
    order = [t[0] for t in THIRDS]
    XA = [Group(x_slice, t, order[t][0], {d: me[d] for d in order[t][1:]}, False) for t in T]
    XB = [Group(x_slice, t, order[t][1], {order[t][2]: me[order[t][2]]}, False) for t in T]
    XC = [Group(x_slice, t, order[t][2], {}, False) for t in T]
    GA = [Group(a_slice, t, order[t][0], {d: me[d] for d in order[t][1:]}, True) for t in T]
    GB = [[Group(a_slice, t, order[t][1], {order[t][0]: shift(order[t][0], o), order[t][2]: me[order[t][2]]}, True) for o in OFF] for t in T]
    GC = [[Group(a_slice, t, order[t][2], {order[t][0]: shift(order[t][0], o), order[t][1]: me[order[t][1]]}, True) for o in OFF] for t in T]
    GL = [[Group(a_slice, t, order[t][2], {order[t][1]: shift(order[t][1], o)}, True) for o in OFF[1:]] for t in T]
    for t in T:
        XA[t].start()
    for t in T:
        GA[t].start()
    for t in T:
        GB[t][0].start()
    for t in T:
        GC[t][0].start()
    for k, i in ((-1, 1), (1, 2)):
        for t in T:
            XA[t].got(k)
        for t in T:
            GA[t].got(k)
        for t in T:
            GB[t][i].start()
        for t in T:
            GC[t][i].start()
    for t in T:
        XA[t].far()
        XB[t].start()
    for k in (-1, 1):
        for t in T:
            GB[t][0].got(k)
    for t in T:
        GA[t].far()
        GB[t][3].start()
    for t in T:
        GC[t][3].start()
    for k in (-1, 1):
        for t in T:
            XB[t].got(k)
    for i in (1, 2):
        for k in (-1, 1):
            for t in T:
                GB[t][i].got(k)
    for t in T:
        XB[t].far()
        XC[t].start()
    for n, k in enumerate((-1, 1)):
        for t in T:
            GB[t][3].got(k)
            GL[t][n].start()
    for i in range(3):
        for k in (-1, 1):
            for t in T:
                GC[t][i].got(k)
    for t in T:
        for i in range(4):
            GB[t][i].far()
        GL[t][2].start()
    for k in (-1, 1):
        for t in T:
            XC[t].got(k)
    for k in (-1, 1):
        for t in T:
            GC[t][3].got(k)
    for i in range(3):
        for k in (-1, 1):
            for t in T:
                GL[t][i].got(k)
    for t in T:
        XC[t].far()
    for f in range(4):
        for h in range(2):
            X[:, 256 * f + 128 * h : 256 * f + 128 * h + 128] = XL[h, :, :, :, 128 * f : 128 * f + 128].reshape(128, 128)
    targets = jnp.concatenate([XL[2, b // 4, b % 4, 0:1, 0:128] for b in range(16)], axis=1)
    row8 = lax.broadcasted_iota(jnp.int32, (8, 1), 0)
    own_rows = (row8 // 2) == c
    block = X[pl.ds(pl.multiple_of((y * 4 + x) * 8, 8), 8), :]
    xi_pair = Pair(jnp.where(own_rows, pltpu.roll(block, lax.rem(2 * c + 8 - 2 * z, 8), 0), 0.0))
    for t in T:
        for g in GC[t] + GL[t]:
            g.far()
    xi = xi_pair.total()

    def a_rows(n, count=2):
        b = n * count
        return A[b // 4, b % 4 : b % 4 + count].reshape(count * 128, 1024)

    def back(weights, position_weights):
        l = stacked(weights, 2)
        p = stacked(position_weights, 2)
        total = nn(l, A[...].reshape(2048, 1024)) + nn(p, XP[0]) + nn(p, XP[1])
        return folded(total, 2)

    def forward(v):
        l = stacked(v, 2)
        rows = jnp.concatenate([folded(nt(l, a_rows(n)), 2) for n in range(8)], axis=1)
        along = folded(nt(l, XP[0]), 2) + folded(nt(l, XP[1]), 2)
        return rows, jnp.sum(xi * v, axis=1, keepdims=True) - along

    diag = lax.broadcasted_iota(jnp.int32, (128, 128), 0) == lax.broadcasted_iota(jnp.int32, (128, 128), 1)
    pick = lax.broadcasted_iota(jnp.int32, (16, 256), 0) == lax.broadcasted_iota(jnp.int32, (16, 256), 1) // 16
    live = row8 < 4

    for newton in range(2):
        xv = X[...]
        for k, piece in enumerate(pieces(xv, 3)):
            XP[k] = piece
        xl3 = stacked(xi, 3)
        inner = folded(nt(xl3, XP[0]), 3) + folded(nt(xl3[:16], XP[1]), 2) + nt(xl3[:8], XP[2])
        sq_col = jnp.sum(lane_parts(xv * xv), axis=1, keepdims=True)
        sq_j = jnp.sum(jnp.where(diag, sq_col, 0.0), axis=0, keepdims=True)
        sq_i = jnp.sum(lane_parts(xi * xi), axis=1, keepdims=True)
        K = jnp.where(live, jnp.exp(-(sq_i + sq_j - 2.0 * inner) / SCALE), 0.0)
        K2 = K * K
        Kx = folded(nn(stacked(K, 3), EX[...]), 3)
        K2x = Kx * Kx
        logit_parts = []
        for n in range(8):
            l = jnp.concatenate([XP[k, 16 * n : 16 * n + 16] for k in range(3)], axis=0)
            g = nt(l, a_rows(n))
            g = g[:16] + g[16:32] + g[32:]
            logit_parts.append(jnp.sum(jnp.where(pick, g, 0.0), axis=0, keepdims=True))
        logits = jnp.concatenate(logit_parts, axis=1)
        prob = 1.0 / (1.0 + jnp.exp(-logits))
        pull = 4.0 * (targets - prob)
        curve = 4.0 * prob * (1.0 - prob)
        k_total = jnp.sum(K, axis=1, keepdims=True)
        k2_total = jnp.sum(K2, axis=1, keepdims=True)
        b_part = (back(Kx * pull, (-0.05 - 2.0 / SCALE) * K) + (2.0 / SCALE) * k_total * xi) / COUNT
        b = Pair(b_part).total()

        def rings(G):
            if newton == 1:
                return Ring("z", lambda k: G.at[:, pl.ds(pl.multiple_of(k * 8, 8), 8)]), (), ()
            zr = Ring("z", lambda k: G.at[:, y, x, pl.ds(pl.multiple_of(k * 8, 8), 8)])
            p2 = [Ring("x", lambda k: G.at[0, y, k]), Ring("y", lambda k: G.at[1, k, x])]
            p3 = [Ring("y", lambda k: G.at[0, k]), Ring("x", lambda k: G.at[1, :, k])]
            return zr, p2, p3

        def put(G, v):
            two = jnp.where(c == 0, v[0:2], v[2:4])
            for p in range(2):
                for f in range(4):
                    for h in range(2):
                        piece = two[p : p + 1, 256 * f + 128 * h : 256 * f + 128 * h + 128]
                        if newton == 0:
                            G[h, y, x, pl.ds(z * 8 + p * 4 + f, 1), :] = piece
                        else:
                            G[h, pl.ds(z * 8 + p * 4 + f, 1), :] = piece

        Bs, Ws = (BG, WG) if newton == 0 else (BL, WL)
        put(Bs, b)
        bz, b2, b3 = rings(Bs)
        bz.start()
        P1, Y1 = forward(b)
        KY = K2 * Y1
        w_part = (back(K2x * curve * P1, -CROSS * KY) + 0.05 * k2_total * b + CROSS * jnp.sum(KY, axis=1, keepdims=True) * xi) / COUNT
        w_pair = Pair(w_part)
        bz.wait()
        if newton == 0:
            for r in b2:
                r.start()
        w = w_pair.total()
        put(Ws, w)
        wz, w2, w3 = rings(Ws)
        wz.start()
        P2, Y2 = forward(w)
        mine = jnp.where(own_rows, 1.0, 0.0)
        quad = lane_parts(K2x * curve * P2 * P2) + CROSS * K2 * Y2 * Y2 + 0.05 * k2_total * lane_parts(w * w)
        rows = [lane_parts(mine * b * b), lane_parts(mine * b * w), lane_parts(mine * w * w), quad / COUNT]
        rows = [jnp.sum(r, axis=0, keepdims=True) for r in rows]
        tile = Pair(jnp.concatenate(rows + [jnp.zeros((4, 128), F32)], axis=0)).total()
        if newton == 0:
            for r in b2:
                r.wait()
            for r in b3:
                r.start()
        wz.wait()
        if newton == 0:
            for r in w2:
                r.start()
        for ph, dim in enumerate(("z", "x", "y")):
            ph += 3 * newton
            SC[ph, me[dim]] = tile
            ring = Ring(dim, lambda k, ph=ph: SC.at[ph, k])
            ring.start()
            ring.wait()
            tile = SC[ph, 0] + SC[ph, 1] + SC[ph, 2] + SC[ph, 3]
            if newton == 0 and ph == 0:
                for r in w2:
                    r.wait()
                for r in w3:
                    r.start()
        tot = jnp.sum(tile, axis=1, keepdims=True)
        rr, bw, ww, wu = (tot[k : k + 1] for k in range(4))
        a0 = rr / bw
        nxt = rr - 2.0 * a0 * bw + a0 * a0 * ww
        beta = nxt / rr
        den = (1.0 + beta) * (1.0 + beta) * bw - 2.0 * (1.0 + beta) * a0 * ww + a0 * a0 * wu
        a1 = nxt / den
        cb = a0 + a1 * (1.0 + beta)
        cw = -a1 * a0
        for h in range(2):
            at = (h, y, x, pl.ds(z, 8, stride=4), slice(None)) if newton == 0 else (h, pl.ds(z, 8, stride=4), slice(None))
            out_ref[newton, :, 128 * h : 128 * h + 128] = cb * Bs[at] + cw * Ws[at]
        if newton == 0:
            for r in b3 + w3:
                r.wait()
            hb, hw = 0.5 * cb, 0.5 * cw
            for blk in range(16):
                for f in range(4):
                    for h in range(2):
                        rows8 = slice(8 * blk, 8 * blk + 8)
                        cols = slice(256 * f + 128 * h, 256 * f + 128 * h + 128)
                        at = (h, blk // 4, blk % 4, pl.ds(f, 8, stride=4), slice(None))
                        X[rows8, cols] = X[rows8, cols] + (hb * BG[at] + hw * WG[at])
            xi = xi + (hb * b + hw * w)
    for d in pending:
        d.wait_send()


def newton_steps(a, xl):
    return pl.pallas_call(
        kernel,
        out_shape=jax.ShapeDtypeStruct((2, 8, 256), F32),
        in_specs=[pl.BlockSpec(memory_space=pl.ANY)] * 2,
        out_specs=pl.BlockSpec(memory_space=pltpu.VMEM),
        scratch_shapes=[
            pltpu.VMEM((4, 4, 8, 16, 1024), BF16),
            pltpu.VMEM((3, 4, 4, 8, 512), F32),
            pltpu.VMEM((128, 1024), F32),
            pltpu.VMEM((3, 128, 1024), BF16),
            pltpu.VMEM((128, 2048), BF16),
            pltpu.VMEM((2, 4, 4, 32, 128), F32),
            pltpu.VMEM((2, 4, 4, 32, 128), F32),
            pltpu.VMEM((2, 32, 128), F32),
            pltpu.VMEM((2, 32, 128), F32),
            pltpu.VMEM((7, 8, 1024), F32),
            pltpu.VMEM((7, 8, 1024), F32),
            pltpu.VMEM((6, 4, 8, 128), F32),
            pltpu.SemaphoreType.DMA((4,)),
            pltpu.SemaphoreType.DMA((NSEM,)),
            pltpu.SemaphoreType.DMA((NSEM,)),
        ],
        compiler_params=pltpu.CompilerParams(collective_id=0, has_side_effects=True, vmem_limit_bytes=60 << 20),
        name="newton_steps",
    )(a, xl)


def per_device(particles, data_rows, labels):
    lab = jnp.broadcast_to(labels.astype(F32).reshape(1, 128), (8, 128))
    xl = jnp.stack([particles[:, :128], particles[:, 128:], lab])
    return newton_steps(data_rows, xl)


def solution(mesh):
    torus = Mesh(mesh.devices.reshape(4, 4, 2, mesh.shape["dim"]), AX)
    return jax.shard_map(
        per_device, mesh=torus, in_specs=(P(DOM, "dim"), P(DOM, None, "dim"), P(DOM, None)),
        out_specs=P(None, DOM, "dim"), check_vma=False,
    )
```
